32 devices in a mesh: row: 8 (over y, x, core), col: 4 (over z).
Axes of the slice: x: 2, y: 2, z: 4, core: 2. Of those that a mesh axis runs over, the one named last changes fastest.
Arguments:
- residual: float32 [2048, 2048], P('row', 'col'), may hold values from -0.15625 to 0.15625
- direction: float32 [2048, 2048], P('row', 'col'), may hold values from -6 to 6
- ground_shift: float32 [1], replicated, may hold values from 1.6937256e-06 to 6.7749024e-06
- previous: float32 [1], replicated, may hold values from 192 to 768
Outputs:
- next_direction: float32 [2048, 2048], P('row', 'col')
- step_ratio: float32 [1], replicated
The draws below stay inside these ranges and needn't reach their ends.
All inputs are finite; a program needn't handle non-finite values.
Results may differ from the reference program's by a relative error of at most 0.00015.
Values sent between devices are 32-bit elements; how exact they have to be, the bound alone decides.
A program may use at most 64 MiB of HBM per device.

```python
import math
import jax
import jax.numpy as jnp
from jax import lax

Q0 = 256
NX = 2048
NY = 2048


def draw_residual(key, part):
    subkeys = jax.random.split(jax.random.fold_in(key, 17), 2)
    row_place = jnp.arange(NX, dtype=jnp.int32).astype(jnp.float32) / NX
    col_scale = jnp.exp(jax.random.uniform(subkeys[1], (NY,), jnp.float32, 0.0, jnp.log(10.0)))
    base_scale = 0.1 / Q0
    row_scale = jnp.exp(row_place * jnp.log(10.0))
    samples = jnp.clip(jax.random.normal(subkeys[0], (NX, NY), jnp.float32), -4.0, 4.0)
    return base_scale * row_scale[:, None] * col_scale[None, :] * samples


def shard_levels(key, dims, cuts, low, largest):
    level = 1.0
    for axis_at, blocks in cuts:
        steps = jax.random.uniform(jax.random.fold_in(jax.random.fold_in(key, 6), axis_at), (blocks,), jnp.float32, low / len(cuts), largest / len(cuts))
        level = level * jnp.repeat(jnp.exp(steps), dims[axis_at] // blocks).reshape((-1,) + (1,) * (len(dims) - 1 - axis_at))
    return level


def gaussian(rng, dims, scale, reach, pieces=(), held_as=jnp.bfloat16):
    result = jax.random.normal(rng, dims, jnp.float32) * scale
    if len(pieces) > 0:
        result = shard_levels(rng, dims, pieces, -0.22, 0.18) * result
    return jnp.clip(result, min=-reach, max=reach).astype(held_as)


def setup_inputs(seed: int = 0) -> dict:
    streams_of = jax.random.split(jax.random.key(seed), 5)
    residual = draw_residual(jax.random.fold_in(streams_of[4], 71), 0)
    direction = gaussian(streams_of[1], (NX, NY), 1.0, 6.0, ((0, 8), (1, 4)), jnp.float32)
    ground_shift = jnp.clip(jnp.exp(jax.random.uniform(streams_of[2], (1,), jnp.float32, math.log(1.6937256077653728e-06), math.log(6.774902431061491e-06))), 1.6937256077653728e-06, 6.774902431061491e-06)
    previous = jnp.clip(jnp.exp(jax.random.uniform(streams_of[3], (1,), jnp.float32, math.log(192.0), math.log(768.0))), 192.0, 768.0)
    return dict(residual=residual, direction=direction, ground_shift=ground_shift, previous=previous)


PRECISE = lax.Precision.HIGHEST

def cosine_matrix(length):
    wavenum = jnp.arange(length, dtype=jnp.int32)[:, None]
    position = jnp.arange(length, dtype=jnp.int32)[None, :]
    phases = wavenum * (2 * position + 1) % (4 * length)
    angles = jnp.pi * phases.astype(jnp.float32) / (2 * length)
    scaling = jnp.where(wavenum == 0, jnp.sqrt(1.0 / length), jnp.sqrt(2.0 / length)).astype(jnp.float32)
    return scaling * jnp.cos(angles)

def reference(residual, direction, ground_shift, previous):
    rows_table = cosine_matrix(NX)
    cols_table = cosine_matrix(NY)
    spectrum = jnp.dot(jnp.dot(rows_table, residual, precision=PRECISE), cols_table.T, precision=PRECISE)
    row_waves = jnp.arange(NX, dtype=jnp.int32).astype(jnp.float32)
    col_waves = jnp.arange(NY, dtype=jnp.int32).astype(jnp.float32)
    row_sine = jnp.sin(jnp.pi * row_waves / (2 * NX))
    col_sine = jnp.sin(jnp.pi * col_waves / (2 * NY))
    eigenvalue = 4.0 * (row_sine * row_sine)[:, None] + 4.0 * (col_sine * col_sine)[None, :]
    weight = 1.0 / (eigenvalue + ground_shift[0])
    scaled = weight * spectrum
    precond = jnp.dot(jnp.dot(rows_table.T, scaled, precision=PRECISE), cols_table, precision=PRECISE)
    inner_total = jnp.sum(residual * precond)
    step_ratio = inner_total / previous[0]
    return (precond + step_ratio * direction, jnp.reshape(step_ratio, (1,)))
```

```python
import functools
import math

import jax
import jax.numpy as jnp
import numpy as np
from jax import lax
from jax.experimental import pallas as pl
from jax.experimental.pallas import tpu as pltpu
from jax.sharding import PartitionSpec as P

MESH = pl.DeviceIdType.MESH


def base_tables(extent, devices):
    length = extent * devices
    half = extent // 2
    odd = 2 * np.arange(extent, dtype=np.int64)[:, None] + 1
    steps = 2 * devices * np.arange(half + 1, dtype=np.int64)[None, :]
    coarse = np.pi * (steps * odd % (4 * length)) / (2 * length)
    scale = math.sqrt(2.0 / length)
    cos_a, sin_a = scale * np.cos(coarse), scale * np.sin(coarse)
    lanes = -(-(devices + 1) // 128) * 128
    fine = np.pi * np.arange(lanes, dtype=np.int64)[None, :] * odd / (2 * length)
    coarse_tables = np.stack([cos_a[:, :-1], sin_a[:, :-1], cos_a[:, 1:], sin_a[:, 1:]])
    fine_tables = np.stack([np.cos(fine), np.sin(fine)])
    waves = []
    for t in range(devices):
        second = devices if t == 0 else 2 * devices - t
        waves.append(2 * devices * np.arange(half) + t)
        waves.append(2 * devices * np.arange(half) + second)
    waves = np.concatenate(waves)
    eigen = 4.0 * np.sin(np.pi * waves / (2 * length)) ** 2
    return (
        coarse_tables.astype(np.float32),
        fine_tables.astype(np.float32),
        eigen.astype(np.float32)[None, :],
    )


def mixing(devices):
    target = np.arange(devices)[:, None]
    source = np.arange(devices)[None, :]
    angles = np.pi * (target * source % (2 * devices)) / devices
    parity = np.where(source % 2 == 0, 1.0, -1.0)
    return np.cos(angles), np.where(target > 0, np.sin(angles), parity)


def weighted_sum(coefs, terms):
    total = None
    for coef, term in zip(coefs, terms):
        coef = float(coef)
        if abs(coef) < 1e-12:
            continue
        if abs(coef - 1.0) < 1e-12:
            total = term if total is None else total + term
        elif abs(coef + 1.0) < 1e-12:
            total = -term if total is None else total - term
        else:
            total = coef * term if total is None else total + coef * term
    return total


def split(value):
    high = value.astype(jnp.bfloat16)
    return high, (value - high.astype(jnp.float32)).astype(jnp.bfloat16)


def kernel(
    rows,
    cols,
    residual_ref,
    coarse_ref,
    fine_ref,
    eigen_ref,
    shift_ref,
    previous_ref,
    out_ref,
    ratio_ref,
    out1,
    in1,
    out2,
    in2,
    table_hi,
    table_lo,
    spec,
    field,
    rowsum,
    colsum,
    inner_row,
    inner_col,
    s1,
    r1,
    s2,
    r2,
    s3,
    r3,
    s4,
    r4,
    s5,
    r5,
    s6,
    r6,
):
    me_r = lax.axis_index("row")
    me_c = lax.axis_index("col")
    extent = residual_ref.shape[0]
    width = out1.shape[1]
    half = extent // 2
    total_cols = width * rows * cols
    f32 = jnp.float32
    mix_cos, mix_sin = mixing(rows)

    barrier = pltpu.get_barrier_semaphore()
    for o in range(1, rows):
        pl.semaphore_signal(
            barrier, inc=1, device_id={"row": lax.rem(me_r + o, rows)}, device_id_type=MESH
        )
    for o in range(1, cols):
        pl.semaphore_signal(
            barrier, inc=1, device_id={"col": lax.rem(me_c + o, cols)}, device_id_type=MESH
        )

    def share(axis, me, count, source, landing, send_sems, recv_sems):
        copies = []
        for o in range(1, count):
            to = lax.rem(me + o, count)
            copy = pltpu.make_async_remote_copy(
                src_ref=source(to),
                dst_ref=landing.at[me],
                send_sem=send_sems.at[o - 1],
                recv_sem=recv_sems.at[o - 1],
                device_id={axis: to},
                device_id_type=MESH,
            )
            copy.start()
            copies.append(copy)
        return copies

    for e in range(0, residual_ref.shape[1], 128):
        turned = residual_ref[:, e : e + 128].T
        for i in range(128 // width):
            out1[e // width + i] = turned[i * width : (i + 1) * width]
    pl.semaphore_wait(barrier, rows + cols - 2)
    first = share("row", me_r, rows, lambda to: out1.at[to], in1, s1, r1)
    in1[me_r] = out1[me_r]

    cos_a, sin_a = coarse_ref[0], coarse_ref[1]
    for t in range(rows):
        if t == 0:
            lane = lax.broadcasted_iota(jnp.int32, (extent, half), 1)
            one = jnp.where(lane == 0, math.sqrt(0.5), 1.0) * coarse_ref[0]
            cos_b = fine_ref[0, :, rows : rows + 1]
            sin_b = fine_ref[1, :, rows : rows + 1]
            two = coarse_ref[0] * cos_b - coarse_ref[1] * sin_b
            zero = jnp.zeros_like(one)
            quads = ((one, zero), (zero, two))
        else:
            cos_b = fine_ref[0, :, t : t + 1]
            sin_b = fine_ref[1, :, t : t + 1]
            quads = (
                (
                    coarse_ref[0] * cos_b - coarse_ref[1] * sin_b,
                    coarse_ref[2] * cos_b + coarse_ref[3] * sin_b,
                ),
                (
                    -(coarse_ref[1] * cos_b + coarse_ref[0] * sin_b),
                    coarse_ref[3] * cos_b - coarse_ref[2] * sin_b,
                ),
            )
        for i in range(2):
            for j in range(2):
                high, low = split(quads[i][j])
                at = (t, slice(i * extent, (i + 1) * extent), slice(j * half, (j + 1) * half))
                table_hi[at] = high
                table_lo[at] = low

    alpha = eigen_ref[...] + shift_ref[0]
    h = 0.5 * jnp.sqrt(alpha)
    z = h / (1.0 + jnp.sqrt(1.0 + h * h))
    z2 = z * z
    series = jnp.full_like(z, 1.0 / 23)
    for p in range(21, 0, -2):
        series = series * z2 + 1.0 / p
    theta = 4.0 * z * series
    gain = 0.5 / jnp.sqrt(alpha * (1.0 + 0.25 * alpha))

    def decay(steps):
        return jnp.exp(-theta * steps)

    for copy in first:
        copy.wait_recv()

    place = lax.broadcasted_iota(jnp.int32, (width, extent), 0)
    for t in range(rows):
        lanes = slice(t * extent, (t + 1) * extent)
        pieces = [in1[d] for d in range(rows)]
        real = weighted_sum(mix_cos[t], pieces)
        imag = weighted_sum(mix_sin[t], pieces)
        high, low = split(jnp.concatenate([real, imag], axis=1))
        both = jnp.dot(
            jnp.concatenate([high, low], axis=0), table_hi[t], preferred_element_type=f32
        )
        value = (
            both[:width] + both[width:] + jnp.dot(high, table_lo[t], preferred_element_type=f32)
        )
        spec[:, lanes] = value
        ahead = value
        behind = value
        q = jnp.exp(-theta[:, lanes])
        s = 1
        while s < width:
            ahead = ahead + q * jnp.where(place >= s, pltpu.roll(ahead, s, 0), 0.0)
            behind = behind + q * jnp.where(
                place < width - s, pltpu.roll(behind, width - s, 0), 0.0
            )
            q = q * q
            s *= 2
        field[:, lanes] = ahead + behind - value
        rowsum[me_r, 0:1, lanes] = ahead[width - 1 : width]
        rowsum[me_r, 1:2, lanes] = behind[0:1]
    mine = rowsum.at[me_r]
    second = share("row", me_r, rows, lambda to: mine, rowsum, s2, r2)
    chunk = decay(float(width))
    group = decay(float(width * rows))
    whole = decay(float(total_cols))
    for copy in second:
        copy.wait_recv()

    def carry(sums, count, me, ratio):
        zero = jnp.zeros_like(ratio)
        left, right, at_end, at_start = zero, zero, zero, zero
        for k in range(count):
            a = sums[k, 0:1, :]
            b = sums[count - 1 - k, 1:2, :]
            at_end = ratio * at_end + a
            at_start = ratio * at_start + b
            left = jnp.where(k < me, at_end, left)
            right = jnp.where(count - 1 - k > me, at_start, right)
        return left, right, at_end, at_start

    left_r, right_r, at_end, at_start = carry(rowsum, rows, me_r, chunk)
    colsum[me_c, 0:1, :] = at_end
    colsum[me_c, 1:2, :] = at_start
    mine = colsum.at[me_c]
    third = share("col", me_c, cols, lambda to: mine, colsum, s3, r3)
    up_r = decay((width * me_r).astype(f32))
    down_r = decay((width * (rows - 1 - me_r)).astype(f32))
    up_c = decay((width * rows * me_c).astype(f32))
    down_c = decay((width * rows * (cols - 1 - me_c)).astype(f32))
    for copy in third:
        copy.wait_recv()
    left_c, right_c, at_end, at_start = carry(colsum, cols, me_c, group)
    images = 1.0 / (1.0 - whole * whole)
    left_c = left_c + up_c * ((at_start + whole * at_end) * images)
    right_c = right_c + down_c * ((at_end + whole * at_start) * images)
    left = left_r + up_r * left_c
    right = right_r + down_r * right_c

    fplace = place.astype(f32)
    reals, imags = [], []
    partial = jnp.zeros((1, extent), f32)
    for t in range(rows):
        lanes = slice(t * extent, (t + 1) * extent)
        th = theta[:, lanes]
        value = gain[:, lanes] * (
            field[:, lanes]
            + jnp.exp(-th * (fplace + 1.0)) * left[:, lanes]
            + jnp.exp(-th * (width - fplace)) * right[:, lanes]
        )
        partial = partial + jnp.sum(spec[:, lanes] * value, axis=0, keepdims=True)
        field[:, lanes] = value
    inner_row[me_r] = jnp.broadcast_to(jnp.sum(partial, axis=1, keepdims=True), (8, 128))
    mine = inner_row.at[me_r]
    fourth = share("row", me_r, rows, lambda to: mine, inner_row, s4, r4)
    turn = (((1,), (1,)), ((), ()))
    for t in range(rows):
        lanes = slice(t * extent, (t + 1) * extent)
        high, low = split(field[:, lanes])
        both = lax.dot_general(
            jnp.concatenate([high, low], axis=0), table_hi[t], turn, preferred_element_type=f32
        )
        value = (
            both[:width]
            + both[width:]
            + lax.dot_general(high, table_lo[t], turn, preferred_element_type=f32)
        )
        reals.append(value[:, :extent])
        imags.append(value[:, extent:])
    for d in range(rows):
        out2[d] = weighted_sum(
            list(mix_cos[:, d]) + list(mix_sin[:, d]), reals + imags
        )
    fifth = share("row", me_r, rows, lambda to: out2.at[to], in2, s5, r5)
    in2[me_r] = out2[me_r]
    for copy in fourth:
        copy.wait_recv()
    inner_col[me_c] = jnp.sum(inner_row[...], axis=0)
    mine = inner_col.at[me_c]
    sixth = share("col", me_c, cols, lambda to: mine, inner_col, s6, r6)
    for copy in sixth:
        copy.wait_recv()
    ratio_ref[...] = jnp.sum(inner_col[...], axis=0) / previous_ref[0]
    for copy in fifth:
        copy.wait_recv()
    for e in range(0, out_ref.shape[1], 128):
        turned = jnp.concatenate([in2[e // width + i] for i in range(128 // width)], axis=0)
        out_ref[:, e : e + 128] = turned.T
    for copies in (first, second, third, fourth, fifth, sixth):
        for copy in copies:
            copy.wait_send()


def body(rows, cols, residual, direction, ground_shift, previous):
    extent, here = residual.shape
    width = here // rows
    length = extent * rows
    f32 = jnp.float32
    coarse, fine, eigen = base_tables(extent, rows)
    vmem = pl.BlockSpec(memory_space=pltpu.VMEM)
    smem = pl.BlockSpec(memory_space=pltpu.SMEM)
    dma = pltpu.SemaphoreType.DMA
    per_row, per_col = max(rows - 1, 1), max(cols - 1, 1)
    precond, ratio = pl.pallas_call(
        functools.partial(kernel, rows, cols),
        out_shape=(
            jax.ShapeDtypeStruct((extent, here), f32),
            jax.ShapeDtypeStruct((8, 128), f32),
        ),
        in_specs=[vmem, vmem, vmem, vmem, smem, smem],
        out_specs=(vmem, vmem),
        scratch_shapes=[
            pltpu.VMEM((rows, width, extent), f32),
            pltpu.VMEM((rows, width, extent), f32),
            pltpu.VMEM((rows, width, extent), f32),
            pltpu.VMEM((rows, width, extent), f32),
            pltpu.VMEM((rows, 2 * extent, extent), jnp.bfloat16),
            pltpu.VMEM((rows, 2 * extent, extent), jnp.bfloat16),
            pltpu.VMEM((width, length), f32),
            pltpu.VMEM((width, length), f32),
            pltpu.VMEM((rows, 2, length), f32),
            pltpu.VMEM((cols, 2, length), f32),
            pltpu.VMEM((rows, 8, 128), f32),
            pltpu.VMEM((cols, 8, 128), f32),
            dma((per_row,)),
            dma((per_row,)),
            dma((per_row,)),
            dma((per_row,)),
            dma((per_col,)),
            dma((per_col,)),
            dma((per_row,)),
            dma((per_row,)),
            dma((per_row,)),
            dma((per_row,)),
            dma((per_col,)),
            dma((per_col,)),
        ],
        compiler_params=pltpu.CompilerParams(collective_id=0, has_side_effects=True),
    )(residual, coarse, fine, eigen, ground_shift, previous)
    step_ratio = ratio[0, :1]
    return precond + step_ratio * direction, step_ratio


def solution(mesh):
    return jax.shard_map(
        functools.partial(body, mesh.shape["row"], mesh.shape["col"]),
        mesh=mesh,
        in_specs=(P("row", "col"), P("row", "col"), P(), P()),
        out_specs=(P("row", "col"), P()),
        check_vma=False,
    )
```

```python
import functools
import math

import jax
import jax.numpy as jnp
import numpy as np
from jax import lax
from jax.experimental import pallas as pl
from jax.experimental.pallas import tpu as pltpu
from jax.sharding import PartitionSpec as P

MESH = pl.DeviceIdType.MESH


def base_tables(extent, devices):
    length = extent * devices
    half = extent // 2
    odd = 2 * np.arange(extent, dtype=np.int64)[:, None] + 1
    steps = 2 * devices * np.arange(half + 1, dtype=np.int64)[None, :]
    coarse = np.pi * (steps * odd % (4 * length)) / (2 * length)
    scale = math.sqrt(2.0 / length)
    cos_a, sin_a = scale * np.cos(coarse), scale * np.sin(coarse)
    lanes = -(-(devices + 1) // 128) * 128
    fine = np.pi * np.arange(lanes, dtype=np.int64)[None, :] * odd / (2 * length)
    coarse_tables = np.stack([cos_a[:, :-1], sin_a[:, :-1], cos_a[:, 1:], sin_a[:, 1:]])
    fine_tables = np.stack([np.cos(fine), np.sin(fine)])
    waves = []
    for t in range(devices):
        second = devices if t == 0 else 2 * devices - t
        waves.append(2 * devices * np.arange(half) + t)
        waves.append(2 * devices * np.arange(half) + second)
    waves = np.concatenate(waves)
    eigen = 4.0 * np.sin(np.pi * waves / (2 * length)) ** 2
    return (
        coarse_tables.astype(np.float32),
        fine_tables.astype(np.float32),
        eigen.astype(np.float32)[None, :],
    )


def mixing(devices):
    target = np.arange(devices)[:, None]
    source = np.arange(devices)[None, :]
    angles = np.pi * (target * source % (2 * devices)) / devices
    parity = np.where(source % 2 == 0, 1.0, -1.0)
    return np.cos(angles), np.where(target > 0, np.sin(angles), parity)


def weighted_sum(coefs, terms):
    total = None
    for coef, term in zip(coefs, terms):
        coef = float(coef)
        if abs(coef) < 1e-12:
            continue
        if abs(coef - 1.0) < 1e-12:
            total = term if total is None else total + term
        elif abs(coef + 1.0) < 1e-12:
            total = -term if total is None else total - term
        else:
            total = coef * term if total is None else total + coef * term
    return total


def split(value):
    high = value.astype(jnp.bfloat16)
    return high, (value - high.astype(jnp.float32)).astype(jnp.bfloat16)


def kernel(
    rows,
    cols,
    residual_hbm,
    direction_hbm,
    coarse_hbm,
    fine_hbm,
    eigen_ref,
    shift_ref,
    previous_ref,
    out_hbm,
    ratio_ref,
    residual_ref,
    direction_ref,
    coarse_ref,
    fine_ref,
    out_ref,
    load_sems,
    store_sems,
    out1,
    in1,
    out2,
    in2,
    table_hi,
    table_lo,
    field,
    from_left,
    from_right,
    own_hi,
    own_lo,
    carried_hi,
    carried_lo,
    rowsum,
    colsum,
    carry,
    s1,
    r1,
    s2,
    r2,
    s3,
    r3,
    s5,
    r5,
):
    me_r = lax.axis_index("row")
    me_c = lax.axis_index("col")
    extent = residual_ref.shape[0]
    width = out1.shape[1]
    half = extent // 2
    total_cols = width * rows * cols
    f32 = jnp.float32
    mix_cos, mix_sin = mixing(rows)

    barrier = pltpu.get_barrier_semaphore()
    for o in range(1, rows):
        pl.semaphore_signal(
            barrier, inc=1, device_id={"row": lax.rem(me_r + o, rows)}, device_id_type=MESH
        )
    for o in range(1, cols):
        pl.semaphore_signal(
            barrier, inc=1, device_id={"col": lax.rem(me_c + o, cols)}, device_id_type=MESH
        )

    loads = []
    for i, (source, landing) in enumerate(
        (
            (residual_hbm, residual_ref),
            (coarse_hbm, coarse_ref),
            (fine_hbm, fine_ref),
            (direction_hbm, direction_ref),
        )
    ):
        copy = pltpu.make_async_copy(source, landing, load_sems.at[i])
        copy.start()
        loads.append(copy)

    def share(axis, me, count, source, landing, send_sems, recv_sems):
        copies = []
        for o in range(1, count):
            to = lax.rem(me + o, count)
            copy = pltpu.make_async_remote_copy(
                src_ref=source(to),
                dst_ref=landing.at[me],
                send_sem=send_sems.at[o - 1],
                recv_sem=recv_sems.at[o - 1],
                device_id={axis: to},
                device_id_type=MESH,
            )
            copy.start()
            copies.append(copy)
        return copies

    loads[0].wait()
    for e in range(0, residual_ref.shape[1], 128):
        turned = residual_ref[:, e : e + 128].T
        for i in range(128 // width):
            out1[e // width + i] = turned[i * width : (i + 1) * width]
    pl.semaphore_wait(barrier, rows + cols - 2)
    first = share("row", me_r, rows, lambda to: out1.at[to], in1, s1, r1)
    in1[me_r] = out1[me_r]

    loads[1].wait()
    loads[2].wait()

    def quadrants(t):
        if t == 0:
            lane = lax.broadcasted_iota(jnp.int32, (extent, half), 1)
            one = jnp.where(lane == 0, math.sqrt(0.5), 1.0) * coarse_ref[0]
            cos_b = fine_ref[0, :, rows : rows + 1]
            sin_b = fine_ref[1, :, rows : rows + 1]
            two = coarse_ref[0] * cos_b - coarse_ref[1] * sin_b
            zero = jnp.zeros_like(one)
            return ((one, zero), (zero, two))
        cos_b = fine_ref[0, :, t : t + 1]
        sin_b = fine_ref[1, :, t : t + 1]
        return (
            (
                coarse_ref[0] * cos_b - coarse_ref[1] * sin_b,
                coarse_ref[2] * cos_b + coarse_ref[3] * sin_b,
            ),
            (
                -(coarse_ref[1] * cos_b + coarse_ref[0] * sin_b),
                coarse_ref[3] * cos_b - coarse_ref[2] * sin_b,
            ),
        )

    for t in range(rows):
        quads = quadrants(t)
        for i in range(2):
            for j in range(2):
                high, low = split(quads[i][j])
                at = (t, slice(i * extent, (i + 1) * extent), slice(j * half, (j + 1) * half))
                table_hi[at] = high
                table_lo[at] = low

    alpha = eigen_ref[...] + shift_ref[...]
    h = 0.5 * jnp.sqrt(alpha)
    z = h / (1.0 + jnp.sqrt(1.0 + h * h))
    z2 = z * z
    series = jnp.full_like(z, 1.0 / 23)
    for p in range(21, 0, -2):
        series = series * z2 + 1.0 / p
    theta = 4.0 * z * series
    gain = 0.5 / jnp.sqrt(alpha * (1.0 + 0.25 * alpha))

    q_one = jnp.exp(-theta)
    place = lax.broadcasted_iota(jnp.int32, (width, extent), 0)
    fplace = place.astype(f32)
    for t in range(rows):
        lanes = slice(t * extent, (t + 1) * extent)
        from_left[:, lanes] = gain[:, lanes] * jnp.exp(-theta[:, lanes] * (fplace + 1.0))
        from_right[:, lanes] = gain[:, lanes] * jnp.exp(-theta[:, lanes] * (width - fplace))
    chunk = jnp.exp(-theta * float(width))
    group = jnp.exp(-theta * float(width * rows))
    whole = jnp.exp(-theta * float(total_cols))

    for copy in first:
        copy.wait_recv()

    length = rows * extent
    partial = jnp.zeros((1, extent), f32)
    for t in range(rows):
        lanes = slice(t * extent, (t + 1) * extent)
        pieces = [in1[d] for d in range(rows)]
        real = weighted_sum(mix_cos[t], pieces)
        imag = weighted_sum(mix_sin[t], pieces)
        high, low = split(jnp.concatenate([real, imag], axis=1))
        both = jnp.dot(
            jnp.concatenate([high, low], axis=0), table_hi[t], preferred_element_type=f32
        )
        value = (
            both[:width] + both[width:] + jnp.dot(high, table_lo[t], preferred_element_type=f32)
        )
        ahead = value
        behind = value
        q = q_one[:, lanes]
        s = 1
        while s < width:
            ahead = ahead + q * jnp.where(place >= s, pltpu.roll(ahead, s, 0), 0.0)
            behind = behind + q * jnp.where(
                place < width - s, pltpu.roll(behind, width - s, 0), 0.0
            )
            q = q * q
            s *= 2
        solved = gain[:, lanes] * (ahead + behind - value)
        partial = partial + jnp.sum(value * solved, axis=0, keepdims=True)
        field[:, lanes] = solved
        rowsum[me_r, 0:1, lanes] = ahead[width - 1 : width]
        rowsum[me_r, 1:2, lanes] = behind[0:1]

    def fold(row):
        return sum(row[:, i : i + 128] for i in range(0, row.shape[1], 128))

    spare = slice(length, length + 128)
    rowsum[me_r, 0:1, spare] = fold(partial)
    rowsum[me_r, 1:2, spare] = jnp.zeros((1, 128), f32)
    mine = rowsum.at[me_r]
    second = share("row", me_r, rows, lambda to: mine, rowsum, s2, r2)

    turn = (((1,), (1,)), ((), ()))
    reals, imags = [], []
    for t in range(rows):
        lanes = slice(t * extent, (t + 1) * extent)
        high, low = split(field[:, lanes])
        both = lax.dot_general(
            jnp.concatenate([high, low], axis=0), table_hi[t], turn, preferred_element_type=f32
        )
        value = (
            both[:width]
            + both[width:]
            + lax.dot_general(high, table_lo[t], turn, preferred_element_type=f32)
        )
        reals.append(value[:, :extent])
        imags.append(value[:, extent:])
    for d in range(rows):
        out2[d] = weighted_sum(list(mix_cos[:, d]) + list(mix_sin[:, d]), reals + imags)
    fifth = share("row", me_r, rows, lambda to: out2.at[to], in2, s5, r5)
    in2[me_r] = out2[me_r]
    for copy in second:
        copy.wait_recv()

    def carries(sums, count, ratio):
        left, right = [jnp.zeros_like(ratio)], [jnp.zeros_like(ratio)]
        for k in range(count):
            left.append(ratio * left[-1] + sums[k, 0:1, :length])
            right.append(ratio * right[-1] + sums[count - 1 - k, 1:2, :length])
        return left[:-1], right[count - 1 :: -1], left[-1], right[-1]

    weight = gain * q_one
    lefts, rights, at_end, at_start = carries(rowsum, rows, chunk)
    coupled = jnp.zeros_like(weight)
    inner = jnp.zeros((1, 128), f32)
    for k in range(rows):
        carry[k, 0:1, :] = lefts[k]
        carry[k, 1:2, :] = rights[k]
        coupled = coupled + lefts[k] * rowsum[k, 1:2, :length] + rights[k] * rowsum[k, 0:1, :length]
        inner = inner + rowsum[k, 0:1, spare]
    colsum[me_c, 0:1, :length] = at_end
    colsum[me_c, 1:2, :length] = at_start
    colsum[me_c, 0:1, spare] = inner + fold(weight * coupled)
    colsum[me_c, 1:2, spare] = jnp.zeros((1, 128), f32)
    mine_c = colsum.at[me_c]
    third = share("col", me_c, cols, lambda to: mine_c, colsum, s3, r3)

    for t in range(rows):
        quads = quadrants(t)
        cos_d, sin_d = f32(mix_cos[t, 0]), f32(mix_sin[t, 0])
        for d in range(1, rows):
            cos_d = jnp.where(me_r == d, f32(mix_cos[t, d]), cos_d)
            sin_d = jnp.where(me_r == d, f32(mix_sin[t, d]), sin_d)
        for j in range(2):
            high, low = split(cos_d * quads[0][j] + sin_d * quads[1][j])
            lanes = slice(t * extent + j * half, t * extent + (j + 1) * half)
            own_hi[:, lanes] = high
            own_lo[:, lanes] = low
    for copy in third:
        copy.wait_recv()

    lefts, rights, at_end, at_start = carries(colsum, cols, group)
    images = 1.0 / (1.0 - whole * whole)
    entry = (at_start + whole * at_end) * images
    exit_ = (at_end + whole * at_start) * images
    for k in range(cols):
        lefts[k] = lefts[k] + entry
        rights[cols - 1 - k] = rights[cols - 1 - k] + exit_
        entry, exit_ = entry * group, exit_ * group
    coupled = jnp.zeros_like(weight)
    inner = jnp.zeros((1, 128), f32)
    left_c, right_c = lefts[0], rights[0]
    for k in range(cols):
        left_c = jnp.where(me_c == k, lefts[k], left_c)
        right_c = jnp.where(me_c == k, rights[k], right_c)
        coupled = coupled + lefts[k] * colsum[k, 1:2, :length] + rights[k] * colsum[k, 0:1, :length]
        inner = inner + colsum[k, 0:1, spare]
    inner = jnp.sum(inner + fold(weight * coupled), axis=1, keepdims=True)
    ratio = inner / previous_ref[...]
    ratio_ref[...] = jnp.broadcast_to(ratio, ratio_ref.shape)
    for k in range(rows):
        carry[k, 0:1, :] = carry[k, 0:1, :] + left_c
        carry[rows - 1 - k, 1:2, :] = carry[rows - 1 - k, 1:2, :] + right_c
        left_c, right_c = left_c * chunk, right_c * chunk

    per = 128 // width
    added = []
    for e in range(0, out_ref.shape[1], 128):
        for k in range(per):
            at = slice(e + k * width, e + (k + 1) * width)
            for t in range(rows):
                lanes = slice(t * extent, (t + 1) * extent)
                r = e // width + k
                high, low = split(
                    from_left[:, lanes] * carry[r, 0:1, lanes]
                    + from_right[:, lanes] * carry[r, 1:2, lanes]
                )
                carried_hi[at, lanes] = high
                carried_lo[at, lanes] = low
        at = slice(e, e + 128)
        added.append(
            lax.dot_general(carried_hi[at, :], own_hi[...], turn, preferred_element_type=f32)
            + lax.dot_general(carried_lo[at, :], own_hi[...], turn, preferred_element_type=f32)
            + lax.dot_general(carried_hi[at, :], own_lo[...], turn, preferred_element_type=f32)
        )
    for copy in fifth:
        copy.wait_recv()
    loads[3].wait()
    stores = []
    for e in range(0, out_ref.shape[1], 128):
        turned = jnp.concatenate([in2[e // width + i] for i in range(per)], axis=0)
        turned = turned + added[e // 128]
        out_ref[:, e : e + 128] = turned.T + ratio * direction_ref[:, e : e + 128]
        copy = pltpu.make_async_copy(
            out_ref.at[:, e : e + 128], out_hbm.at[:, e : e + 128], store_sems.at[e // 128]
        )
        copy.start()
        stores.append(copy)
    for copy in stores:
        copy.wait()
    for copies in (first, second, third, fifth):
        for copy in copies:
            copy.wait_send()


def body(rows, cols, residual, direction, ground_shift, previous):
    extent, here = residual.shape
    width = here // rows
    length = extent * rows
    f32 = jnp.float32
    coarse, fine, eigen = base_tables(extent, rows)
    vmem = pl.BlockSpec(memory_space=pltpu.VMEM)
    smem = pl.BlockSpec(memory_space=pltpu.SMEM)
    dma = pltpu.SemaphoreType.DMA
    per_row, per_col = max(rows - 1, 1), max(cols - 1, 1)
    anywhere = pl.BlockSpec(memory_space=pl.ANY)
    output, ratio = pl.pallas_call(
        functools.partial(kernel, rows, cols),
        out_shape=(
            jax.ShapeDtypeStruct((extent, here), f32),
            jax.ShapeDtypeStruct((1, 1), f32),
        ),
        in_specs=[anywhere, anywhere, anywhere, anywhere, vmem, vmem, vmem],
        out_specs=(anywhere, vmem),
        scratch_shapes=[
            pltpu.VMEM((extent, here), f32),
            pltpu.VMEM((extent, here), f32),
            pltpu.VMEM(coarse.shape, f32),
            pltpu.VMEM(fine.shape, f32),
            pltpu.VMEM((extent, here), f32),
            dma((4,)),
            dma((here // 128,)),
            pltpu.VMEM((rows, width, extent), f32),
            pltpu.VMEM((rows, width, extent), f32),
            pltpu.VMEM((rows, width, extent), f32),
            pltpu.VMEM((rows, width, extent), f32),
            pltpu.VMEM((rows, 2 * extent, extent), jnp.bfloat16),
            pltpu.VMEM((rows, 2 * extent, extent), jnp.bfloat16),
            pltpu.VMEM((width, length), f32),
            pltpu.VMEM((width, length), f32),
            pltpu.VMEM((width, length), f32),
            pltpu.VMEM((extent, length), jnp.bfloat16),
            pltpu.VMEM((extent, length), jnp.bfloat16),
            pltpu.VMEM((here, length), jnp.bfloat16),
            pltpu.VMEM((here, length), jnp.bfloat16),
            pltpu.VMEM((rows, 2, length + 128), f32),
            pltpu.VMEM((cols, 2, length + 128), f32),
            pltpu.VMEM((rows, 2, length), f32),
            dma((per_row,)),
            dma((per_row,)),
            dma((per_row,)),
            dma((per_row,)),
            dma((per_col,)),
            dma((per_col,)),
            dma((per_row,)),
            dma((per_row,)),
        ],
        compiler_params=pltpu.CompilerParams(collective_id=0, has_side_effects=True),
    )(residual, direction, coarse, fine, eigen, ground_shift.reshape(1, 1), previous.reshape(1, 1))
    return output, ratio.reshape(1)


def solution(mesh):
    return jax.shard_map(
        functools.partial(body, mesh.shape["row"], mesh.shape["col"]),
        mesh=mesh,
        in_specs=(P("row", "col"), P("row", "col"), P(), P()),
        out_specs=(P("row", "col"), P()),
        check_vma=False,
    )
```

```python
import functools
import math

import jax
import jax.numpy as jnp
import numpy as np
from jax import lax
from jax.experimental import pallas as pl
from jax.experimental.pallas import tpu as pltpu
from jax.sharding import PartitionSpec as P

MESH = pl.DeviceIdType.MESH


def base_tables(extent, devices):
    length = extent * devices
    half = extent // 2
    odd = 2 * np.arange(extent, dtype=np.int64)[:, None] + 1
    steps = 2 * devices * np.arange(half + 1, dtype=np.int64)[None, :]
    coarse = np.pi * (steps * odd % (4 * length)) / (2 * length)
    scale = math.sqrt(2.0 / length)
    cos_a, sin_a = scale * np.cos(coarse), scale * np.sin(coarse)
    lanes = -(-(devices + 1) // 128) * 128
    fine = np.pi * np.arange(lanes, dtype=np.int64)[None, :] * odd / (2 * length)
    coarse_tables = np.stack([cos_a[:, :-1], sin_a[:, :-1], cos_a[:, 1:], sin_a[:, 1:]])
    fine_tables = np.stack([np.cos(fine), np.sin(fine)])
    waves = []
    for t in range(devices):
        second = devices if t == 0 else 2 * devices - t
        waves.append(2 * devices * np.arange(half) + t)
        waves.append(2 * devices * np.arange(half) + second)
    waves = np.concatenate(waves)
    eigen = 4.0 * np.sin(np.pi * waves / (2 * length)) ** 2
    return (
        coarse_tables.astype(np.float32),
        fine_tables.astype(np.float32),
        eigen.astype(np.float32)[None, :],
    )


def mixing(devices):
    target = np.arange(devices)[:, None]
    source = np.arange(devices)[None, :]
    angles = np.pi * (target * source % (2 * devices)) / devices
    parity = np.where(source % 2 == 0, 1.0, -1.0)
    return np.cos(angles), np.where(target > 0, np.sin(angles), parity)


def weighted_sum(coefs, terms):
    total = None
    for coef, term in zip(coefs, terms):
        coef = float(coef)
        if abs(coef) < 1e-12:
            continue
        if abs(coef - 1.0) < 1e-12:
            total = term if total is None else total + term
        elif abs(coef + 1.0) < 1e-12:
            total = -term if total is None else total - term
        else:
            total = coef * term if total is None else total + coef * term
    return total


def split(value):
    high = value.astype(jnp.bfloat16)
    return high, (value - high.astype(jnp.float32)).astype(jnp.bfloat16)


def kernel(
    rows,
    cols,
    residual_hbm,
    direction_hbm,
    coarse_hbm,
    fine_hbm,
    eigen_ref,
    shift_ref,
    previous_ref,
    out_hbm,
    ratio_ref,
    residual_ref,
    direction_ref,
    coarse_ref,
    fine_ref,
    out_ref,
    load_sems,
    store_sems,
    out1,
    in1,
    out2,
    in2,
    table_hi,
    table_lo,
    field,
    from_left,
    from_right,
    own_hi,
    own_lo,
    carried_hi,
    carried_lo,
    added,
    rowsum,
    colsum,
    carry,
    s1,
    r1,
    s2,
    r2,
    s3,
    r3,
    s5,
    r5,
):
    me_r = lax.axis_index("row")
    me_c = lax.axis_index("col")
    extent = residual_ref.shape[0]
    width = out1.shape[1]
    half = extent // 2
    total_cols = width * rows * cols
    f32 = jnp.float32
    mix_cos, mix_sin = mixing(rows)

    barrier = pltpu.get_barrier_semaphore()
    for o in range(1, rows):
        pl.semaphore_signal(
            barrier, inc=1, device_id={"row": lax.rem(me_r + o, rows)}, device_id_type=MESH
        )
    for o in range(1, cols):
        pl.semaphore_signal(
            barrier, inc=1, device_id={"col": lax.rem(me_c + o, cols)}, device_id_type=MESH
        )

    loads = []
    for i, (source, landing) in enumerate(
        (
            (residual_hbm, residual_ref),
            (coarse_hbm, coarse_ref),
            (fine_hbm, fine_ref),
            (direction_hbm, direction_ref),
        )
    ):
        copy = pltpu.make_async_copy(source, landing, load_sems.at[i])
        copy.start()
        loads.append(copy)

    def share(axis, me, count, source, landing, send_sems, recv_sems):
        copies = []
        for o in range(1, count):
            to = lax.rem(me + o, count)
            copy = pltpu.make_async_remote_copy(
                src_ref=source(to),
                dst_ref=landing.at[me],
                send_sem=send_sems.at[o - 1],
                recv_sem=recv_sems.at[o - 1],
                device_id={axis: to},
                device_id_type=MESH,
            )
            copy.start()
            copies.append(copy)
        return copies

    loads[0].wait()
    for e in range(0, residual_ref.shape[1], 128):
        turned = residual_ref[:, e : e + 128].T
        for i in range(128 // width):
            out1[e // width + i] = turned[i * width : (i + 1) * width]
    pl.semaphore_wait(barrier, rows + cols - 2)
    first = share("row", me_r, rows, lambda to: out1.at[to], in1, s1, r1)
    in1[me_r] = out1[me_r]

    loads[1].wait()
    loads[2].wait()

    def quadrants(t):
        if t == 0:
            lane = lax.broadcasted_iota(jnp.int32, (extent, half), 1)
            one = jnp.where(lane == 0, math.sqrt(0.5), 1.0) * coarse_ref[0]
            cos_b = fine_ref[0, :, rows : rows + 1]
            sin_b = fine_ref[1, :, rows : rows + 1]
            two = coarse_ref[0] * cos_b - coarse_ref[1] * sin_b
            zero = jnp.zeros_like(one)
            return ((one, zero), (zero, two))
        cos_b = fine_ref[0, :, t : t + 1]
        sin_b = fine_ref[1, :, t : t + 1]
        return (
            (
                coarse_ref[0] * cos_b - coarse_ref[1] * sin_b,
                coarse_ref[2] * cos_b + coarse_ref[3] * sin_b,
            ),
            (
                -(coarse_ref[1] * cos_b + coarse_ref[0] * sin_b),
                coarse_ref[3] * cos_b - coarse_ref[2] * sin_b,
            ),
        )

    for t in range(rows):
        quads = quadrants(t)
        for i in range(2):
            for j in range(2):
                high, low = split(quads[i][j])
                at = (t, slice(i * extent, (i + 1) * extent), slice(j * half, (j + 1) * half))
                table_hi[at] = high
                table_lo[at] = low

    alpha = eigen_ref[...] + shift_ref[...]
    h = 0.5 * jnp.sqrt(alpha)
    z = h / (1.0 + jnp.sqrt(1.0 + h * h))
    z2 = z * z
    series = jnp.full_like(z, 1.0 / 23)
    for p in range(21, 0, -2):
        series = series * z2 + 1.0 / p
    theta = 4.0 * z * series
    gain = 0.5 / jnp.sqrt(alpha * (1.0 + 0.25 * alpha))

    q_one = jnp.exp(-theta)
    place = lax.broadcasted_iota(jnp.int32, (width, extent), 0)
    fplace = place.astype(f32)
    for t in range(rows):
        lanes = slice(t * extent, (t + 1) * extent)
        from_left[:, lanes] = gain[:, lanes] * jnp.exp(-theta[:, lanes] * (fplace + 1.0))
        from_right[:, lanes] = gain[:, lanes] * jnp.exp(-theta[:, lanes] * (width - fplace))
    chunk = jnp.exp(-theta * float(width))
    group = jnp.exp(-theta * float(width * rows))
    whole = jnp.exp(-theta * float(total_cols))

    for copy in first:
        copy.wait_recv()

    length = rows * extent
    partial = jnp.zeros((1, extent), f32)
    for t in range(rows):
        lanes = slice(t * extent, (t + 1) * extent)
        pieces = [in1[d] for d in range(rows)]
        real = weighted_sum(mix_cos[t], pieces)
        imag = weighted_sum(mix_sin[t], pieces)
        high, low = split(jnp.concatenate([real, imag], axis=1))
        both = jnp.dot(
            jnp.concatenate([high, low], axis=0), table_hi[t], preferred_element_type=f32
        )
        value = (
            both[:width] + both[width:] + jnp.dot(high, table_lo[t], preferred_element_type=f32)
        )
        ahead = value
        behind = value
        q = q_one[:, lanes]
        s = 1
        while s < width:
            ahead = ahead + q * jnp.where(place >= s, pltpu.roll(ahead, s, 0), 0.0)
            behind = behind + q * jnp.where(
                place < width - s, pltpu.roll(behind, width - s, 0), 0.0
            )
            q = q * q
            s *= 2
        solved = gain[:, lanes] * (ahead + behind - value)
        partial = partial + jnp.sum(value * solved, axis=0, keepdims=True)
        field[:, lanes] = solved
        rowsum[me_r, 0:1, lanes] = ahead[width - 1 : width]
        rowsum[me_r, 1:2, lanes] = behind[0:1]

    def fold(row):
        return sum(row[:, i : i + 128] for i in range(0, row.shape[1], 128))

    spare = slice(length, length + 128)
    rowsum[me_r, 0:1, spare] = fold(partial)
    rowsum[me_r, 1:2, spare] = jnp.zeros((1, 128), f32)
    mine = rowsum.at[me_r]
    second = share("row", me_r, rows, lambda to: mine, rowsum, s2, r2)

    turn = (((1,), (1,)), ((), ()))
    reals, imags = [], []
    for t in range(rows):
        lanes = slice(t * extent, (t + 1) * extent)
        high, low = split(field[:, lanes])
        both = lax.dot_general(
            jnp.concatenate([high, low], axis=0), table_hi[t], turn, preferred_element_type=f32
        )
        value = (
            both[:width]
            + both[width:]
            + lax.dot_general(high, table_lo[t], turn, preferred_element_type=f32)
        )
        reals.append(value[:, :extent])
        imags.append(value[:, extent:])
    for d in range(rows):
        out2[d] = weighted_sum(list(mix_cos[:, d]) + list(mix_sin[:, d]), reals + imags)
    fifth = share("row", me_r, rows, lambda to: out2.at[to], in2, s5, r5)
    in2[me_r] = out2[me_r]
    for copy in second:
        copy.wait_recv()

    def carries(sums, count, ratio):
        left, right = [jnp.zeros_like(ratio)], [jnp.zeros_like(ratio)]
        for k in range(count):
            left.append(ratio * left[-1] + sums[k, 0:1, :length])
            right.append(ratio * right[-1] + sums[count - 1 - k, 1:2, :length])
        return left[:-1], right[count - 1 :: -1], left[-1], right[-1]

    weight = gain * q_one
    lefts, rights, at_end, at_start = carries(rowsum, rows, chunk)
    coupled = jnp.zeros_like(weight)
    inner = jnp.zeros((1, 128), f32)
    for k in range(rows):
        carry[k, 0:1, :] = lefts[k]
        carry[k, 1:2, :] = rights[k]
        coupled = coupled + lefts[k] * rowsum[k, 1:2, :length] + rights[k] * rowsum[k, 0:1, :length]
        inner = inner + rowsum[k, 0:1, spare]
    colsum[me_c, 0:1, :length] = at_end
    colsum[me_c, 1:2, :length] = at_start
    colsum[me_c, 0:1, spare] = inner + fold(weight * coupled)
    colsum[me_c, 1:2, spare] = jnp.zeros((1, 128), f32)
    mine_c = colsum.at[me_c]
    third = share("col", me_c, cols, lambda to: mine_c, colsum, s3, r3)

    for t in range(rows):
        quads = quadrants(t)
        cos_d, sin_d = f32(mix_cos[t, 0]), f32(mix_sin[t, 0])
        for d in range(1, rows):
            cos_d = jnp.where(me_r == d, f32(mix_cos[t, d]), cos_d)
            sin_d = jnp.where(me_r == d, f32(mix_sin[t, d]), sin_d)
        for j in range(2):
            high, low = split(cos_d * quads[0][j] + sin_d * quads[1][j])
            lanes = slice(t * extent + j * half, t * extent + (j + 1) * half)
            own_hi[:, lanes] = high
            own_lo[:, lanes] = low
    for copy in third:
        copy.wait_recv()

    lefts, rights, at_end, at_start = carries(colsum, cols, group)
    images = 1.0 / (1.0 - whole * whole)
    entry = (at_start + whole * at_end) * images
    exit_ = (at_end + whole * at_start) * images
    for k in range(cols):
        lefts[k] = lefts[k] + entry
        rights[cols - 1 - k] = rights[cols - 1 - k] + exit_
        entry, exit_ = entry * group, exit_ * group
    coupled = jnp.zeros_like(weight)
    inner = jnp.zeros((1, 128), f32)
    left_c, right_c = lefts[0], rights[0]
    for k in range(cols):
        left_c = jnp.where(me_c == k, lefts[k], left_c)
        right_c = jnp.where(me_c == k, rights[k], right_c)
        coupled = coupled + lefts[k] * colsum[k, 1:2, :length] + rights[k] * colsum[k, 0:1, :length]
        inner = inner + colsum[k, 0:1, spare]
    inner = jnp.sum(inner + fold(weight * coupled), axis=1, keepdims=True)
    ratio = inner / previous_ref[...]
    ratio_ref[...] = jnp.broadcast_to(ratio, ratio_ref.shape)
    for k in range(rows):
        carry[k, 0:1, :] = carry[k, 0:1, :] + left_c
        carry[rows - 1 - k, 1:2, :] = carry[rows - 1 - k, 1:2, :] + right_c
        left_c, right_c = left_c * chunk, right_c * chunk

    per = 128 // width
    block = out_ref.shape[1]
    for e in range(0, out_ref.shape[1], block):
        for r in range(e // width, (e + block) // width):
            at = slice(r * width, (r + 1) * width)
            for t in range(rows):
                lanes = slice(t * extent, (t + 1) * extent)
                high, low = split(
                    from_left[:, lanes] * carry[r, 0:1, lanes]
                    + from_right[:, lanes] * carry[r, 1:2, lanes]
                )
                carried_hi[at, lanes] = high
                carried_lo[at, lanes] = low
        at = slice(e, e + block)
        added[at, :] = (
            lax.dot_general(carried_hi[at, :], own_hi[...], turn, preferred_element_type=f32)
            + lax.dot_general(carried_lo[at, :], own_hi[...], turn, preferred_element_type=f32)
            + lax.dot_general(carried_hi[at, :], own_lo[...], turn, preferred_element_type=f32)
        )
    for copy in fifth:
        copy.wait_recv()
    loads[3].wait()
    stores = []
    for e in range(0, out_ref.shape[1], 128):
        turned = jnp.concatenate([in2[e // width + i] for i in range(per)], axis=0)
        turned = turned + added[e : e + 128, :]
        out_ref[:, e : e + 128] = turned.T + ratio * direction_ref[:, e : e + 128]
        copy = pltpu.make_async_copy(
            out_ref.at[:, e : e + 128], out_hbm.at[:, e : e + 128], store_sems.at[e // 128]
        )
        copy.start()
        stores.append(copy)
    for copy in stores:
        copy.wait()
    for copies in (first, second, third, fifth):
        for copy in copies:
            copy.wait_send()


def body(rows, cols, residual, direction, ground_shift, previous):
    extent, here = residual.shape
    width = here // rows
    length = extent * rows
    f32 = jnp.float32
    coarse, fine, eigen = base_tables(extent, rows)
    vmem = pl.BlockSpec(memory_space=pltpu.VMEM)
    smem = pl.BlockSpec(memory_space=pltpu.SMEM)
    dma = pltpu.SemaphoreType.DMA
    per_row, per_col = max(rows - 1, 1), max(cols - 1, 1)
    anywhere = pl.BlockSpec(memory_space=pl.ANY)
    output, ratio = pl.pallas_call(
        functools.partial(kernel, rows, cols),
        out_shape=(
            jax.ShapeDtypeStruct((extent, here), f32),
            jax.ShapeDtypeStruct((1, 1), f32),
        ),
        in_specs=[anywhere, anywhere, anywhere, anywhere, vmem, vmem, vmem],
        out_specs=(anywhere, vmem),
        scratch_shapes=[
            pltpu.VMEM((extent, here), f32),
            pltpu.VMEM((extent, here), f32),
            pltpu.VMEM(coarse.shape, f32),
            pltpu.VMEM(fine.shape, f32),
            pltpu.VMEM((extent, here), f32),
            dma((4,)),
            dma((here // 128,)),
            pltpu.VMEM((rows, width, extent), f32),
            pltpu.VMEM((rows, width, extent), f32),
            pltpu.VMEM((rows, width, extent), f32),
            pltpu.VMEM((rows, width, extent), f32),
            pltpu.VMEM((rows, 2 * extent, extent), jnp.bfloat16),
            pltpu.VMEM((rows, 2 * extent, extent), jnp.bfloat16),
            pltpu.VMEM((width, length), f32),
            pltpu.VMEM((width, length), f32),
            pltpu.VMEM((width, length), f32),
            pltpu.VMEM((extent, length), jnp.bfloat16),
            pltpu.VMEM((extent, length), jnp.bfloat16),
            pltpu.VMEM((here, length), jnp.bfloat16),
            pltpu.VMEM((here, length), jnp.bfloat16),
            pltpu.VMEM((here, extent), f32),
            pltpu.VMEM((rows, 2, length + 128), f32),
            pltpu.VMEM((cols, 2, length + 128), f32),
            pltpu.VMEM((rows, 2, length), f32),
            dma((per_row,)),
            dma((per_row,)),
            dma((per_row,)),
            dma((per_row,)),
            dma((per_col,)),
            dma((per_col,)),
            dma((per_row,)),
            dma((per_row,)),
        ],
        compiler_params=pltpu.CompilerParams(collective_id=0, has_side_effects=True),
    )(residual, direction, coarse, fine, eigen, ground_shift.reshape(1, 1), previous.reshape(1, 1))
    return output, ratio.reshape(1)


def solution(mesh):
    return jax.shard_map(
        functools.partial(body, mesh.shape["row"], mesh.shape["col"]),
        mesh=mesh,
        in_specs=(P("row", "col"), P("row", "col"), P(), P()),
        out_specs=(P("row", "col"), P()),
        check_vma=False,
    )
```
